32 devices in a mesh: mem: 4 (over y, core), lat: 4 (over z), lon: 2 (over x).
Axes of the slice: x: 2, y: 2, z: 4, core: 2. Of those that a mesh axis runs over, the one named last changes fastest.
Arguments:
- fields: bfloat16 [4, 2, 96, 96, 512], P('mem', None, 'lat', 'lon'), may hold values from -6 to 6
- region: int32 [96, 96], P('lat', 'lon'), may hold values from 0 to 2
- gain_attn: float32 [512], replicated, may hold values from 0.1 to 1.9
- w_qkv: bfloat16 [512, 1536], P(None, ('mem', 'lat', 'lon')), may hold values from -1 to 1
- w_proj: bfloat16 [512, 512], P(None, ('mem', 'lat', 'lon')), may hold values from -0.25 to 0.25
- gain_mlp: float32 [512], replicated, may hold values from 0.1 to 1.9
- w_up: bfloat16 [512, 2048], P(None, ('mem', 'lat', 'lon')), may hold values from -0.25 to 0.25
- w_down: bfloat16 [2048, 512], P(None, ('mem', 'lat', 'lon')), may hold values from -0.125 to 0.125
Outputs:
- updated: bfloat16 [4, 2, 96, 96, 512], P('mem', None, 'lat', 'lon')
The draws below stay inside these ranges and needn't reach their ends.
All inputs are finite; a program needn't handle non-finite values.
Results may differ from the reference program's by a relative error of at most 0.011.
Values may be sent and summed in bfloat16 or wider, within the bound.
A program may use at most 192 MiB of HBM per device.

```python
import jax
import jax.numpy as jnp
from jax import lax

D = 512
HEADS = 16
FF = 2048
HDIM = 32
WLAT = 6
WLON = 12
LEVELS = 2
SH = 3
SL = 6
MEMBERS = 4
NLAT = 96
NLON = 96


def draw_w_qkv(key, part):
    first = jax.random.fold_in(key, 11)
    drawn = jnp.clip(jax.random.normal(first, (D, 3 * D), jnp.float32), -6.0, 6.0) / D ** 0.5
    return drawn.astype(jnp.bfloat16)


def with_ends(array, key, least, top_value):
    shape = array.shape
    index_at = [jax.random.randint(jax.random.fold_in(key, axis), (), 0, shape[axis]) for axis in range(len(shape))]
    array = array.at[tuple(index_at)].set(least)
    longest = shape.index(max(shape))
    index_at[longest] = (index_at[longest] + 1) % shape[longest]
    return array.at[tuple(index_at)].set(top_value)


def levels(own_key, dims, split, low, largest):
    factor_of = 1.0
    for axis_at, blocks in split:
        heights = jax.random.uniform(jax.random.fold_in(jax.random.fold_in(own_key, 6), axis_at), (blocks,), jnp.float32, low / len(split), largest / len(split))
        factor_of = factor_of * jnp.repeat(jnp.exp(heights), dims[axis_at] // blocks).reshape((-1,) + (1,) * (len(dims) - 1 - axis_at))
    return factor_of


def scatter_about(rng, dims, deviation, most, split=(), held_as=jnp.bfloat16):
    drawn = deviation * jax.random.normal(rng, dims, jnp.float32)
    if split:
        drawn = drawn * levels(rng, dims, split, -0.22, 0.18)
    return jnp.clip(drawn, -most, most).astype(held_as)


def setup_inputs(seed: int = 0) -> dict:
    splits = jax.random.split(jax.random.key(seed), 9)
    fields = scatter_about(splits[0], (MEMBERS, LEVELS, NLAT, NLON, D), 1.0, 6.0, ((0, 4), (2, 4), (3, 2)))
    region = with_ends(jax.random.randint(splits[1], (NLAT, NLON), 0, 3), jax.random.fold_in(splits[1], 1), 0, 2).astype(jnp.int32)
    gain_attn = jnp.clip(1.0 + 0.18 * jax.random.normal(splits[2], (D,), jnp.float32), 0.1, 1.9)
    w_qkv = draw_w_qkv(jax.random.fold_in(splits[8], 71), 0)
    w_proj = scatter_about(splits[4], (D, D), D ** -0.5, 0.25, ((1, 32),))
    gain_mlp = jnp.clip(1.0 + 0.18 * jax.random.normal(splits[5], (D,), jnp.float32), 0.1, 1.9)
    w_up = scatter_about(splits[6], (D, FF), D ** -0.5, 0.25, ((1, 32),))
    w_down = scatter_about(splits[7], (FF, D), FF ** -0.5, 0.125, ((1, 32),))
    return dict(fields=fields, region=region, gain_attn=gain_attn, w_qkv=w_qkv, w_proj=w_proj, gain_mlp=gain_mlp, w_up=w_up, w_down=w_down)


eps = 1e-05

def layer_norm(values, gain_vec):
    values = values.astype(jnp.float32)
    average = lax.optimization_barrier(jnp.mean(values, axis=-1, keepdims=True))
    centred = values - average
    variance = lax.optimization_barrier(jnp.mean(centred * centred, axis=-1, keepdims=True))
    return (centred * lax.rsqrt(variance + eps) * gain_vec).astype(jnp.bfloat16)

def to_windows(arr):
    chans = arr.shape[-1]
    arr = arr.reshape(LEVELS, NLAT // WLAT, WLAT, NLON // WLON, WLON, chans)
    arr = arr.transpose(1, 3, 0, 2, 4, 5)
    return arr.reshape(NLAT // WLAT, NLON // WLON, LEVELS * WLAT * WLON, chans)

def reference(fields, region, gain_attn, w_qkv, w_proj, gain_mlp, w_up, w_down):
    scale = 1.0 / HDIM ** 0.5
    win_tok = LEVELS * WLAT * WLON
    shifted_ids = jnp.roll(region, (-SH, -SL), axis=(0, 1)).astype(jnp.int32)
    north = ((jnp.arange(NLAT) + SH) % NLAT < SH).astype(jnp.int32)
    ids_win = to_windows(jnp.broadcast_to(shifted_ids[None, :, :, None], (LEVELS, NLAT, NLON, 1)))[..., 0]
    north_win = to_windows(jnp.broadcast_to(north[None, :, None, None], (LEVELS, NLAT, NLON, 1)))[..., 0]

    def band_fn(args):
        tokens, ids_band, north_band = args
        count = tokens.shape[0]
        qkv_all = jnp.dot(tokens.reshape(-1, D), w_qkv, preferred_element_type=jnp.float32).astype(jnp.bfloat16)
        qkv_all = qkv_all.reshape(count, win_tok, 3, HEADS, HDIM).astype(jnp.float32)
        queries = qkv_all[:, :, 0]
        keys_in = qkv_all[:, :, 1]
        values_in = qkv_all[:, :, 2]
        scores = jnp.einsum('wqhd,wkhd->whqk', queries, keys_in) * scale
        allow = (ids_band[:, :, None] == ids_band[:, None, :]) & (north_band[:, :, None] == north_band[:, None, :])
        scores = jnp.where(allow[:, None], scores, -1000000000.0)
        attn_probs = jax.nn.softmax(scores, axis=-1).astype(jnp.bfloat16)
        mixed_heads = jnp.einsum('whqk,wkhd->wqhd', attn_probs.astype(jnp.float32), values_in).astype(jnp.bfloat16)
        mixed_heads = mixed_heads.reshape(count * win_tok, D)
        projected = jnp.dot(mixed_heads, w_proj, preferred_element_type=jnp.float32).astype(jnp.bfloat16)
        return projected.reshape(count, win_tok, D)

    def one_member(member):
        normed = layer_norm(member, gain_attn)
        shifted = jnp.roll(normed, (-SH, -SL), axis=(1, 2))
        out_win = lax.map(band_fn, (to_windows(shifted), ids_win, north_win))
        out_win = out_win.reshape(NLAT // WLAT, NLON // WLON, LEVELS, WLAT, WLON, D)
        attn_out = out_win.transpose(2, 0, 3, 1, 4, 5).reshape(LEVELS, NLAT, NLON, D)
        attn_out = jnp.roll(attn_out, (SH, SL), axis=(1, 2))
        resid = (member.astype(jnp.float32) + attn_out.astype(jnp.float32)).astype(jnp.bfloat16)
        normed2 = layer_norm(resid, gain_mlp).reshape(-1, D)
        hidden = jax.nn.gelu(jnp.dot(normed2, w_up, preferred_element_type=jnp.float32), approximate=False).astype(jnp.bfloat16)
        delta = jnp.dot(hidden, w_down, preferred_element_type=jnp.float32).reshape(LEVELS, NLAT, NLON, D)
        return (resid.astype(jnp.float32) + delta).astype(jnp.bfloat16)
    return lax.map(one_member, fields)
```

```python
import functools

import jax
import jax.numpy as jnp
from jax import lax
from jax.experimental import pallas as pl
from jax.experimental.pallas import tpu as pltpu
from jax.sharding import PartitionSpec as P

HDIM = 32
WLAT = 6
WLON = 12
SH = 3
SL = 6
LANES = 128
AXES = ("mem", "lat", "lon")
BIG = 1e9
EXP2_SCALE = 1.4426950408889634 / HDIM**0.5

eps = 1e-05

NT = (((1,), (1,)), ((), ()))
TN = (((0,), (0,)), ((), ()))


def dot32(a, b, dims):
    return lax.dot_general(a, b, dims, preferred_element_type=jnp.float32)


def shifted_2(block, axis, distance):
    devices = range(lax.axis_size(axis))
    route = [((i - distance) % len(devices), i) for i in devices]
    return lax.ppermute(block, axis, route)


def norm(values, gain):
    average = jnp.mean(values, axis=-1, keepdims=True)
    centred = values - average
    variance = jnp.mean(centred * centred, axis=-1, keepdims=True)
    return (centred * lax.rsqrt(variance + eps) * gain).astype(jnp.bfloat16)


def pieces(levels, wins):
    for w in range(wins):
        for l in range(levels):
            for r in range(WLAT):
                yield l, r, w * WLON, ((w * levels + l) * WLAT + r) * WLON


def attention_kernel(x_ref, hot_ref, gain_ref, wqkv_ref, wproj_ref, out_ref, grid_s, tok_s, qkv_s, mix_s):
    levels, _, cols, width = x_ref.shape
    wins = cols // WLON
    ntok = levels * WLAT * WLON
    grid_s[...] = x_ref[...].astype(jnp.float32)
    for l, r, c, t in pieces(levels, wins):
        tok_s[pl.ds(t, WLON), :] = grid_s[l, r, pl.ds(c, WLON), :]
    normed = norm(tok_s[...], gain_ref[...])
    for part in range(3):
        at = pl.ds(part * width, width)
        qkv_s[:, at] = dot32(normed, wqkv_ref[at, :], NT).astype(jnp.bfloat16)
    per = LANES // HDIM
    lane_head = lax.broadcasted_iota(jnp.int32, (ntok, LANES), 1) // HDIM
    for w in range(wins):
        rows = pl.ds(w * ntok, ntok)
        hot = hot_ref[0, rows, :]
        barred = ((hot.astype(jnp.float32) - 1.0) * BIG).astype(jnp.bfloat16)
        for g in range(width // LANES):
            q = qkv_s[rows, pl.ds(g * LANES, LANES)]
            k = qkv_s[rows, pl.ds(width + g * LANES, LANES)]
            v = qkv_s[rows, pl.ds(2 * width + g * LANES, LANES)]
            queries = jnp.concatenate(
                [jnp.concatenate([jnp.where(lane_head == h, q, jnp.zeros_like(q)), hot], axis=1) for h in range(per)],
                axis=0,
            )
            keys = jnp.concatenate([k, barred], axis=1)
            scores = dot32(keys, queries, NT)
            top = jnp.max(scores, axis=0, keepdims=True)
            probs = jnp.exp2((scores - top) * EXP2_SCALE)
            total = jnp.sum(probs, axis=0, keepdims=True)
            mixed = dot32(v, probs.astype(jnp.bfloat16), TN) * (1.0 / total)
            heads = [mixed[h * HDIM : (h + 1) * HDIM, h * ntok : (h + 1) * ntok] for h in range(per)]
            mix_s[rows, pl.ds(g * LANES, LANES)] = jnp.concatenate(heads, axis=0).T.astype(jnp.bfloat16)
    attn_out = dot32(mix_s[...], wproj_ref[...], NT).astype(jnp.bfloat16).astype(jnp.float32)
    out_ref[0] = (tok_s[...] + attn_out).astype(jnp.bfloat16)


def mlp_kernel(resid_ref, gain_ref, wup_ref, wdown_ref, out_ref, grid_s, tok_s):
    levels, _, cols, width = out_ref.shape
    hidden_all = wup_ref.shape[0]
    resid = resid_ref[0].astype(jnp.float32)
    normed = norm(resid, gain_ref[...])
    tok_s[...] = resid
    step = min(width, hidden_all)
    for at in range(0, hidden_all, step):
        pre = dot32(normed, wup_ref[pl.ds(at, step), :], NT)
        hidden = (0.5 * pre * (1.0 + lax.erf(pre * 0.5**0.5))).astype(jnp.bfloat16)
        tok_s[...] += dot32(hidden, wdown_ref[:, pl.ds(at, step)], NT)
    for l, r, c, t in pieces(levels, cols // WLON):
        grid_s[l, r, pl.ds(c, WLON), :] = tok_s[pl.ds(t, WLON), :]
    out_ref[...] = grid_s[...].astype(jnp.bfloat16)


def whole(shape):
    return pl.BlockSpec(shape, lambda b: (0,) * len(shape))


def body(fields, region, gain_attn, w_qkv, w_proj, gain_mlp, w_up, w_down):
    member = fields[0]
    levels, clat, clon, width = member.shape
    bands, wins = clat // WLAT, clon // WLON
    ntok = levels * WLAT * WLON
    btok = wins * ntok

    wqkv_t = lax.all_gather(w_qkv.T, AXES, axis=0, tiled=True)
    wproj_t = lax.all_gather(w_proj.T, AXES, axis=0, tiled=True)
    wup_t = lax.all_gather(w_up.T, AXES, axis=0, tiled=True)
    wdown_t = lax.all_gather(w_down.T, AXES, axis=0, tiled=True)

    region_ids = region.astype(jnp.bfloat16)
    row_ids = jnp.arange(clat, dtype=jnp.int32)
    nlat_all = clat * lax.axis_size("lat")
    north_side = (lax.axis_index("lat") * clat + SH + row_ids) % nlat_all < SH
    arrived, arrived_ids = shifted_2((member[:, :SH], region_ids[:SH]), "lat", -1)
    lat_band = jnp.concatenate([member[:, SH:], arrived], axis=1)
    band_ids = jnp.concatenate([region_ids[SH:], arrived_ids], axis=0)
    strip, strip_ids = shifted_2((lat_band[:, :, :SL], band_ids[:, :SL]), "lon", -1)
    shifted = jnp.concatenate([lat_band[:, :, SL:], strip], axis=2)
    shifted_ids = jnp.concatenate([band_ids[:, SL:], strip_ids], axis=1)

    groups = shifted_ids.astype(jnp.int32) + 3 * north_side[:, None].astype(jnp.int32)
    groups = groups.reshape(bands, 1, WLAT, wins, WLON).transpose(0, 3, 1, 2, 4)
    groups = jnp.broadcast_to(groups, (bands, wins, levels, WLAT, WLON)).reshape(bands, btok)
    hot = (groups[:, :, None] == jnp.arange(LANES, dtype=jnp.int32)).astype(jnp.bfloat16)

    grid_block = pl.BlockSpec((levels, WLAT, clon, width), lambda b: (0, b, 0, 0))
    tok_block = pl.BlockSpec((1, btok, width), lambda b: (b, 0, 0))
    f32_scratch = [pltpu.VMEM((levels, WLAT, clon, width), jnp.float32), pltpu.VMEM((btok, width), jnp.float32)]
    count = levels * clat * clon
    params = pltpu.CompilerParams(dimension_semantics=("arbitrary",), vmem_limit_bytes=56 * 2**20)
    resid = pl.pallas_call(
        attention_kernel,
        grid=(bands,),
        in_specs=[
            grid_block,
            pl.BlockSpec((1, btok, LANES), lambda b: (b, 0, 0)),
            whole((1, width)),
            whole(wqkv_t.shape),
            whole(wproj_t.shape),
        ],
        out_specs=tok_block,
        out_shape=jax.ShapeDtypeStruct((bands, btok, width), jnp.bfloat16),
        scratch_shapes=f32_scratch
        + [pltpu.VMEM((btok, 3 * width), jnp.bfloat16), pltpu.VMEM((btok, width), jnp.bfloat16)],
        compiler_params=params,
        cost_estimate=pl.CostEstimate(
            flops=24 * count * width * width // 3, bytes_accessed=4 * count * width, transcendentals=count * 4096
        ),
    )(shifted, hot, gain_attn[None], wqkv_t, wproj_t)
    out = pl.pallas_call(
        mlp_kernel,
        grid=(bands,),
        in_specs=[tok_block, whole((1, width)), whole(wup_t.shape), whole(wdown_t.shape)],
        out_specs=grid_block,
        out_shape=jax.ShapeDtypeStruct(member.shape, jnp.bfloat16),
        scratch_shapes=f32_scratch,
        compiler_params=params,
        cost_estimate=pl.CostEstimate(
            flops=4 * count * width * wup_t.shape[0], bytes_accessed=4 * count * width, transcendentals=count * 2048
        ),
    )(resid, gain_mlp[None], wup_t, wdown_t)

    arrived_cols = shifted_2(out[:, :, clon - SL :], "lon", 1)
    out = jnp.concatenate([arrived_cols, out[:, :, : clon - SL]], axis=2)
    arrived_rows = shifted_2(out[:, clat - SH :], "lat", 1)
    out = jnp.concatenate([arrived_rows, out[:, : clat - SH]], axis=1)
    return out[None]


def solution(mesh):
    columns = P(None, AXES)
    in_specs = (P("mem", None, "lat", "lon", None), P("lat", "lon"), P(), columns, columns, P(), columns, columns)
    out_specs = P("mem", None, "lat", "lon", None)
    return jax.shard_map(body, mesh=mesh, in_specs=in_specs, out_specs=out_specs, check_vma=False)
```
